32 devices in a mesh: smp: 8 (over z, x), feat: 4 (over y, core).
Axes of the slice: x: 2, y: 2, z: 4, core: 2. Of those that a mesh axis runs over, the one named last changes fastest.
Arguments:
- features: float32 [16384, 16384], P('smp', 'feat'), may hold values from -6 to 6
- logits: float32 [16384, 256], P('smp'), may hold values from -500 to 500
- labels: int32 [16384], P('smp'), may hold values from 0 to 255
- direction: float32 [16384, 256], P('feat'), may hold values from -6 to 6
Outputs:
- hess_vec: float32 [16384, 256], P('feat')
- gradient: float32 [16384, 256], P('feat')
The draws below stay inside these ranges and needn't reach their ends.
All inputs are finite; a program needn't handle non-finite values.
Results may differ from the reference program's by a relative error of at most 0.000071.
Values sent between devices are 32-bit elements; how exact they have to be, the bound alone decides.
A program may use at most 128 MiB of HBM per device.

```python
import jax
import jax.numpy as jnp
from jax import lax

F = 16384
C = 256
SAMPLES = 16384


def draw_logits(key, part):
    keys = jax.random.split(key, 3)
    key_shift, key_bias, key_noise = (keys[0], keys[1], keys[2])
    bias = jax.random.uniform(key_bias, (1, C), jnp.float32, -2.0, 0.0)
    noise = jax.random.uniform(key_noise, (SAMPLES, C), jnp.float32, -1.0, 1.0)
    shift = jax.random.normal(key_shift, (SAMPLES, 1), jnp.float32) * 3.0
    base = shift + bias + noise
    return jnp.clip(base, -500.0, 500.0).astype(jnp.float32)


def with_ends(entries, key, low, largest):
    longest = entries.shape.index(max(entries.shape))
    spots = []
    for shift in (0, 1):
        where = [jax.random.randint(jax.random.fold_in(key, axis), (), 0, length) for axis, length in enumerate(entries.shape)]
        where[longest] = (where[longest] + shift) % entries.shape[longest]
        spots.append(tuple(where))
    return entries.at[spots[0]].set(low).at[spots[1]].set(largest)


def shard_levels(own_key, shape, pieces, least, high):
    def one(position, shards_of):
        steps = jax.random.uniform(jax.random.fold_in(jax.random.fold_in(own_key, 6), position), (shards_of,), jnp.float32, least / len(pieces), high / len(pieces))
        return jnp.repeat(jnp.exp(steps), shape[position] // shards_of).reshape((-1,) + (1,) * (len(shape) - position - 1))

    factor_of = one(*pieces[0])
    for cut in pieces[1:]:
        factor_of = factor_of * one(*cut)
    return factor_of


def bell_draw(own_key, extent, scale, reach, cuts=(), kind=jnp.bfloat16):
    gain = shard_levels(own_key, extent, cuts, -0.22, 0.18) if cuts else 1.0
    entries = jax.random.normal(own_key, extent, jnp.float32) * scale * gain
    return jnp.minimum(jnp.maximum(entries, -reach), reach).astype(kind)


def setup_inputs(seed: int = 0) -> dict:
    streams_of = jax.random.split(jax.random.key(seed), 5)
    return {
        "features": jnp.clip(jax.random.uniform(streams_of[0], (SAMPLES, F), jnp.float32, -6.0, 6.0) * shard_levels(streams_of[0], (SAMPLES, F), ((0, 8), (1, 4)), -0.4, 0.0), -6.0, 6.0),
        "logits": draw_logits(jax.random.fold_in(streams_of[4], 71), 0),
        "labels": with_ends(jax.random.randint(streams_of[2], (SAMPLES,), 0, C), jax.random.fold_in(streams_of[2], 1), 0, C - 1).astype(jnp.int32),
        "direction": bell_draw(streams_of[3], (F, C), 1.0, 6.0, ((0, 4),), jnp.float32),
    }


def reference(features, logits, labels, direction):
    samples = features.shape[0]
    classes = direction.shape[1]
    projected = jnp.dot(features, direction, precision=lax.Precision.HIGHEST, preferred_element_type=jnp.float32)
    probs = jax.nn.softmax(logits, axis=1)
    weighted = probs * projected
    curv_rows = (weighted - probs * lax.optimization_barrier(jnp.sum(weighted, axis=1, keepdims=True))) / samples
    onehot = (labels[:, None] == jnp.arange(classes, dtype=jnp.int32)[None, :]).astype(jnp.float32)
    resid_rows = (probs - onehot) / jnp.sqrt(jnp.float32(samples))
    combined = jnp.concatenate([curv_rows, resid_rows], axis=1)
    total = lax.dot_general(features, combined, (((0,), (0,)), ((), ())), precision=lax.Precision.HIGHEST, preferred_element_type=jnp.float32)
    hess_vec = total[:, :classes] + 0.25 * direction
    gradient = total[:, classes:]
    return (hess_vec, gradient)
```

```python
import jax
import jax.numpy as jnp
from jax import lax
from jax.sharding import PartitionSpec as P

HIGH = lax.Precision.HIGH
STREAMS = 4


def products(features, rows):
    return lax.dot_general(
        features, rows, (((0,), (0,)), ((), ())), precision=HIGH, preferred_element_type=jnp.float32
    )


def half(block, which):
    rows = block.shape[0] // 2
    return lax.dynamic_slice_in_dim(block, which * rows, rows, 0)


def joined(mine, other, bit):
    low = jnp.where(bit == 0, mine, other)
    high = jnp.where(bit == 0, other, mine)
    return jnp.concatenate([low, high], axis=0)


def pair_scatter(block, axis):
    size = lax.axis_size(axis)
    bit = lax.axis_index(axis) % 2
    pairs = [(i, i ^ 1) for i in range(size)]
    return half(block, bit) + lax.ppermute(half(block, 1 - bit), axis, pairs)


def pair_gather(block, axis):
    size = lax.axis_size(axis)
    bit = lax.axis_index(axis) % 2
    pairs = [(i, i ^ 1) for i in range(size)]
    return joined(block, lax.ppermute(block, axis, pairs), bit)


def ring(axis, way):
    size = lax.axis_size(axis)
    count = size // 2
    hops = [(i, (i // 2 + way) % count * 2 + i % 2) for i in range(size)]
    return count, lax.axis_index(axis) // 2, hops


def ring_scatter(block, axis, way):
    count, place, hops = ring(axis, way)
    rows = block.shape[0] // count

    def chunk(k):
        return lax.dynamic_slice_in_dim(block, (place - way * k + 2 * count) % count * rows, rows, 0)

    acc = chunk(1)
    for step in range(1, count):
        acc = chunk(1 + step) + lax.ppermute(acc, axis, hops)
    return acc


def ring_gather(block, axis, way):
    count, place, hops = ring(axis, way)
    rows = block.shape[0]
    out = jnp.zeros((count * rows,) + block.shape[1:], block.dtype)
    out = lax.dynamic_update_slice_in_dim(out, block, place * rows, 0)
    for step in range(1, count):
        block = lax.ppermute(block, axis, hops)
        out = lax.dynamic_update_slice_in_dim(out, block, (place - way * step + count) % count * rows, 0)
    return out


def sum_stream(block, axis, kind):
    way = 1 if kind % 2 == 0 else -1
    if kind < 2:
        own = ring_scatter(pair_scatter(block, axis), axis, way)
        return pair_gather(ring_gather(own, axis, way), axis)
    own = pair_scatter(ring_scatter(block, axis, way), axis)
    return ring_gather(pair_gather(own, axis), axis, way)


def sum_feat(block, axis):
    size = lax.axis_size(axis)
    own = pair_scatter(block, axis)
    bit = 2
    while bit < size:
        own = own + lax.ppermute(own, axis, [(i, i ^ bit) for i in range(size)])
        bit *= 2
    return pair_gather(own, axis)


def on_device(features, logits, labels, direction):
    samples = features.shape[0] * lax.axis_size("smp")
    classes = direction.shape[1]
    cols = features.shape[1] // STREAMS
    probs = jax.nn.softmax(logits, axis=1)
    onehot = (labels[:, None] == jnp.arange(classes, dtype=jnp.int32)[None, :]).astype(jnp.float32)
    resid_rows = (probs - onehot) / jnp.sqrt(jnp.float32(samples))

    def parts_of(rows):
        return [products(features[:, k * cols : (k + 1) * cols], rows) for k in range(STREAMS)]

    grad_parts = parts_of(resid_rows)
    *grad_parts, later = lax.optimization_barrier((*grad_parts, direction))
    gradient = jnp.concatenate([sum_stream(g, "smp", k) for k, g in enumerate(grad_parts)], axis=0)
    half_rows = features.shape[0] // 2
    curv = []
    for k in range(2):
        span = slice(k * half_rows, (k + 1) * half_rows)
        partial_u = jnp.dot(features[span], later, precision=HIGH, preferred_element_type=jnp.float32)
        projected = sum_feat(partial_u, "feat")
        weighted = probs[span] * projected
        curv.append((weighted - probs[span] * jnp.sum(weighted, axis=1, keepdims=True)) / samples)
    curv_rows = jnp.concatenate(curv, axis=0)
    hess_parts = parts_of(curv_rows)
    hess = [sum_stream(h, "smp", k) for k, h in enumerate(hess_parts)]
    hess_vec = jnp.concatenate(hess, axis=0) + 0.25 * direction
    return (hess_vec, gradient)


def solution(mesh):
    placed = (P("smp", "feat"), P("smp", None), P("smp"), P("feat", None))
    return jax.shard_map(
        on_device,
        mesh=mesh,
        in_specs=placed,
        out_specs=(P("feat", None), P("feat", None)),
        check_vma=False,
    )
```
